128 devices in a mesh: dp: 16 (over y, x_hi, core), fsdp: 8 (over z, x_lo).
Axes of the slice: x: 4 (x_hi: 2, x_lo: 2; x = x_hi * 2 + x_lo), y: 4, z: 4, core: 2. Of those that a mesh axis runs over, the one named last changes fastest.
Arguments:
- acts: bfloat16 [65536, 8192], P(('dp', 'fsdp')), may hold values from -24 to 24
- grad_out: bfloat16 [65536, 1024], P(('dp', 'fsdp')), may hold values from -24 to 24
- codes: int32 [128, 16, 1024], P('fsdp'), may hold values from 0 to 65535
- scale_codes: int32 [128, 1024], P('fsdp'), may hold values from 0 to 255
- col_scale: float32 [1024], replicated, may hold values from 0.03 to 0.3
- down_adapter: bfloat16 [64, 8192], P(None, 'fsdp'), may hold values from -0.1796875 to 0.1796875
- up_adapter: bfloat16 [64, 1024], P(None, 'fsdp'), may hold values from -0.1875 to 0.1875
Outputs:
- input_gradient: bfloat16 [65536, 8192], P(('dp', 'fsdp'))
- grad_down: float32 [64, 8192], P(None, 'fsdp')
- grad_up: float32 [64, 1024], P(None, 'fsdp')
The draws below stay inside these ranges and needn't reach their ends.
All inputs are finite; a program needn't handle non-finite values.
Results may differ from the reference program's by a relative error of at most 0.0059.
Values may be sent and summed in bfloat16 or wider, within the bound.
No kernel may reach another device: no remote copies, remote signals or barrier semaphores. Data moves between devices by JAX's collectives and lax.ppermute only.
A program may use at most 128 MiB of HBM per device.

```python
import math
import jax
import jax.numpy as jnp
from jax import lax

D = 8192
O = 1024
R = 64
TOK_DEV = 512
TOKEN_TOTAL = 65536


def touch_ends(array, own_key, smallest, top_value):
    longest = array.shape.index(max(array.shape))
    spots = []
    for shift in (0, 1):
        where = [jax.random.randint(jax.random.fold_in(own_key, axis), (), 0, length) for axis, length in enumerate(array.shape)]
        where[longest] = (where[longest] + shift) % array.shape[longest]
        spots.append(tuple(where))
    return array.at[spots[0]].set(smallest).at[spots[1]].set(top_value)


def strengthened(result, key, source, target, blocks, factor):
    def block_of(dim):
        return (jnp.arange(result.shape[dim]) // (result.shape[dim] // blocks)).reshape((-1,) + (1,) * (result.ndim - 1 - dim))

    first = jax.random.permutation(key, blocks)[block_of(target)]
    far = (block_of(target) + blocks // 2) % blocks
    return jnp.where((block_of(source) == first) | (block_of(source) == far), factor * result, result)


def block_levels(key, shape, cuts, smallest, largest):
    def one(dim, shards_of):
        steps = jax.random.uniform(jax.random.fold_in(jax.random.fold_in(key, 6), dim), (shards_of,), jnp.float32, smallest / len(cuts), largest / len(cuts))
        return jnp.repeat(jnp.exp(steps), shape[dim] // shards_of).reshape((-1,) + (1,) * (len(shape) - dim - 1))

    level = one(*cuts[0])
    for cut in cuts[1:]:
        level = level * one(*cut)
    return level


def bell_draw(stream_key, extent, width, bound, cuts=(), kind=jnp.bfloat16):
    result = width * jax.random.normal(stream_key, extent, jnp.float32)
    if cuts:
        result = result * block_levels(stream_key, extent, cuts, -0.22, 0.18)
    return jnp.clip(result, -bound, bound).astype(kind)


def gaussian_with(stream_key, shape, deviation, limit, pieces, heavy, dtype=jnp.bfloat16):
    drawn = deviation * jax.random.normal(stream_key, shape, jnp.float32)
    if pieces:
        drawn = drawn * block_levels(stream_key, shape, pieces, -0.22, 0.18)
    return jnp.clip(strengthened(drawn, jax.random.fold_in(stream_key, 3), *heavy), -limit, limit).astype(dtype)


def setup_inputs(seed: int = 0) -> dict:
    arg_keys = jax.random.split(jax.random.key(seed), 8)
    acts = gaussian_with(arg_keys[0], (TOKEN_TOTAL, D), 1.0, 24.0, ((0, 128),), (0, 1, 128, 5.5))
    grad_out = gaussian_with(arg_keys[1], (TOKEN_TOTAL, O), 1.0, 24.0, ((0, 128),), (0, 1, 128, 5.5))
    codes = touch_ends(jax.random.randint(arg_keys[2], (D // 64, 16, O), 0, 65536), jax.random.fold_in(arg_keys[2], 1), 0, 65535).astype(jnp.int32)
    scale_codes = touch_ends(jax.random.randint(arg_keys[3], (D // 64, O), 0, 256), jax.random.fold_in(arg_keys[3], 1), 0, 255).astype(jnp.int32)
    col_scale = jnp.clip(jnp.exp(jax.random.uniform(arg_keys[4], (O,), jnp.float32, math.log(0.03), math.log(0.3))), 0.03, 0.3)
    down_adapter = bell_draw(arg_keys[5], (R, D), 0.03, 0.1796875, ((1, 8),))
    up_adapter = bell_draw(arg_keys[6], (R, O), O ** -0.5, 0.1875, ((1, 8),))
    return {"acts": acts, "grad_out": grad_out, "codes": codes, "scale_codes": scale_codes, "col_scale": col_scale, "down_adapter": down_adapter, "up_adapter": up_adapter}


adapter_scale = 0.5
nf4_table = [-1.0, -0.6961928009986877, -0.5250730514526367, -0.39491748809814453, -0.28444138169288635, -0.18477343022823334, -0.09105003625154495, 0.0, 0.07958029955625534, 0.16093020141124725, 0.24611230194568634, 0.33791524171829224, 0.44070982933044434, 0.5626170039176941, 0.7229568362236023, 1.0]


def dequantize(codes, scale_codes, col_scale):
    block_count = codes.shape[0]
    columns = codes.shape[2]
    nibbles = jnp.stack([(codes >> (4 * nibble_pos)) & 15 for nibble_pos in range(4)], axis=2)
    levels = jnp.zeros(nibbles.shape, jnp.float32)
    for position, quantum in enumerate(nf4_table):
        levels = jnp.where(nibbles == position, jnp.float32(quantum), levels)
    absmax = (scale_codes.astype(jnp.float32) + 1.0) / 256.0 * col_scale[None, :]
    weight = levels * absmax[:, None, None, :]
    return weight.reshape(block_count * 64, columns).astype(jnp.bfloat16)


def reference(acts, grad_out, codes, scale_codes, col_scale, down_adapter, up_adapter):
    weight = dequantize(codes, scale_codes, col_scale)
    blocks_in = acts.reshape(TOKEN_TOTAL // TOK_DEV, TOK_DEV, D)
    blocks_out = grad_out.reshape(TOKEN_TOTAL // TOK_DEV, TOK_DEV, O)
    scale_factor = adapter_scale * TOKEN_TOTAL ** -0.5

    def one_block(carry, pair):
        act_rows, grad_rows = pair
        mixed = jnp.dot(grad_rows, up_adapter.T, preferred_element_type=jnp.float32).astype(jnp.bfloat16)
        lowered = jnp.dot(act_rows, down_adapter.T, preferred_element_type=jnp.float32).astype(jnp.bfloat16)
        frozen_base = lax.dot_general(grad_rows, weight, (((1,), (1,)), ((), ())), preferred_element_type=jnp.float32)
        operand_side = jnp.dot(mixed, down_adapter, preferred_element_type=jnp.float32)
        incoming_gradient_rows = (frozen_base + adapter_scale * operand_side).astype(jnp.bfloat16)
        term_down = lax.dot_general(mixed, act_rows, (((0,), (0,)), ((), ())), preferred_element_type=jnp.float32)
        term_up = lax.dot_general(lowered, grad_rows, (((0,), (0,)), ((), ())), preferred_element_type=jnp.float32)
        return (carry[0] + term_down, carry[1] + term_up), incoming_gradient_rows

    start = (jnp.zeros((R, D), jnp.float32), jnp.zeros((R, O), jnp.float32))
    totals, grad_blocks = lax.scan(one_block, start, (blocks_in, blocks_out))
    input_gradient = grad_blocks.reshape(TOKEN_TOTAL, D)
    return input_gradient, scale_factor * totals[0], scale_factor * totals[1]
```

```python
import functools

import jax
import jax.numpy as jnp
from jax import lax
from jax.experimental import pallas as pl
from jax.experimental.pallas import tpu as pltpu
from jax.sharding import Mesh
from jax.sharding import PartitionSpec as P


adapter_scale = 0.5
nf4_table = [
    -1.0,
    -0.6961928009986877,
    -0.5250730514526367,
    -0.39491748809814453,
    -0.28444138169288635,
    -0.18477343022823334,
    -0.09105003625154495,
    0.0,
    0.07958029955625534,
    0.16093020141124725,
    0.24611230194568634,
    0.33791524171829224,
    0.44070982933044434,
    0.5626170039176941,
    0.7229568362236023,
    1.0,
]

AXES = ("y", "xh", "core", "z", "xl")
SIZES = (4, 2, 2, 4, 2)
DEVICES = 128
HALF = 512
SHARD = 1024
WIDTH = 8192
COLS = 1024
TOKENS = 512
RANK_HALF = 32
PACKED = 1152
FSDP = 8


def place(device):
    rest, xl = divmod(device, 2)
    rest, z = divmod(rest, 4)
    rest, core = divmod(rest, 2)
    y, xh = divmod(rest, 2)
    return xh * 2 + xl, y, z, core


def device_at(x, y, z, core):
    return (((y * 2 + x // 2) * 2 + core) * 4 + z) * 2 + x % 2


def z_hop(x, y, z, core):
    step = 1 if (core + y) % 2 == 0 else -1
    return x, y, (z + step) % 4, core


def x_hop(x, y, z, core):
    step = 1 if core == 0 else -1
    return (x + step) % 4, y, z, core


def y_swap(x, y, z, core):
    step = 1 if (core + y) % 2 == 0 else -1
    return x, (y + step) % 4, z, core


def core_swap(x, y, z, core):
    return x, y, z, 1 - core


def moved(value, hop):
    pairs = [(d, device_at(*hop(*place(d)))) for d in range(DEVICES)]
    return lax.ppermute(value, AXES, pairs)


def dequant_kernel(core_ref, codes_ref, scale_ref, col_ref, out_ref, rows_ref):
    step = pl.program_id(0)
    for b in range(2):
        absmax = scale_ref[pl.ds(step * 2 + b, 1), :].astype(jnp.float32)
        absmax = (absmax + 1.0) / 256.0 * col_ref[...]
        words = codes_ref[b]
        for j in range(4):
            bits = [(words & (1 << (4 * j + k))) != 0 for k in range(4)]
            levels = [jnp.full(words.shape, q, jnp.float32) for q in nf4_table]
            for k in range(4):
                levels = [
                    jnp.where(bits[k], levels[i + 1], levels[i])
                    for i in range(0, len(levels), 2)
                ]
            value = levels[0] * absmax
            for lane in range(COLS // 128):
                rows_ref[lane, pl.ds(b * 64 + j, 16, stride=4), :] = value[
                    :, lane * 128 : (lane + 1) * 128
                ]
    for lane in range(COLS // 128):
        out_ref[:, lane * 128 : (lane + 1) * 128] = rows_ref[lane].astype(jnp.bfloat16)


def dequantized_half(core, codes, scale_codes, col_scale):
    return pl.pallas_call(
        dequant_kernel,
        grid_spec=pltpu.PrefetchScalarGridSpec(
            num_scalar_prefetch=1,
            grid=(4,),
            in_specs=[
                pl.BlockSpec((2, 16, COLS), lambda i, c: (c[0] * 4 + i, 0, 0)),
                pl.BlockSpec((8, COLS), lambda i, c: (c[0], 0)),
                pl.BlockSpec((1, COLS), lambda i, c: (0, 0)),
            ],
            out_specs=pl.BlockSpec((128, COLS), lambda i, c: (i, 0)),
            scratch_shapes=[pltpu.VMEM((COLS // 128, 128, 128), jnp.float32)],
        ),
        out_shape=jax.ShapeDtypeStruct((HALF, COLS), jnp.bfloat16),
        cost_estimate=pl.CostEstimate(
            flops=2_000_000_000, bytes_accessed=1_600_000, transcendentals=0
        ),
        name="dequant",
    )(core, codes, scale_codes, col_scale.reshape(1, COLS))


NT = (((1,), (1,)), ((), ()))
TN = (((0,), (0,)), ((), ()))


def adapter_kernel(
    grad_ref, acts_ref, own_ref, other_ref, mixed_ref, sum_own_ref, sum_other_ref, lowered_ref
):
    f = pl.program_id(0)

    @pl.when(f == 0)
    def _():
        for side, ref in enumerate((own_ref, other_ref)):
            total = jnp.zeros((TOKENS, RANK_HALF), jnp.float32)
            for g in range(FSDP):
                total += lax.dot_general(
                    grad_ref[:, g * 128 : (g + 1) * 128],
                    ref[g, :, SHARD:],
                    NT,
                    preferred_element_type=jnp.float32,
                )
            mixed_ref[:, side * RANK_HALF : (side + 1) * RANK_HALF] = total.astype(jnp.bfloat16)
        lowered_ref[...] = jnp.zeros_like(lowered_ref)

    acts = acts_ref[...]
    down = jnp.concatenate([own_ref[f, :, :SHARD], other_ref[f, :, :SHARD]], axis=0)
    lowered_ref[...] += lax.dot_general(acts, down, NT, preferred_element_type=jnp.float32)
    term = lax.dot_general(mixed_ref[...], acts, TN, preferred_element_type=jnp.float32)
    sum_own_ref[f, :, :SHARD] = term[:RANK_HALF].astype(jnp.bfloat16)
    sum_other_ref[f, :, :SHARD] = term[RANK_HALF:].astype(jnp.bfloat16)

    @pl.when(f == FSDP - 1)
    def _():
        lowered = lowered_ref[...].astype(jnp.bfloat16)
        term_up = lax.dot_general(lowered, grad_ref[...], TN, preferred_element_type=jnp.float32)
        term_up = term_up.astype(jnp.bfloat16)
        for g in range(FSDP):
            part = term_up[:, g * 128 : (g + 1) * 128]
            sum_own_ref[g, :, SHARD:] = part[:RANK_HALF]
            sum_other_ref[g, :, SHARD:] = part[RANK_HALF:]


def adapter_terms(grad_out, acts, own, other):
    whole = pl.BlockSpec((FSDP, RANK_HALF, PACKED), lambda f: (0, 0, 0))
    packed = jax.ShapeDtypeStruct((FSDP, RANK_HALF, PACKED), jnp.bfloat16)
    return pl.pallas_call(
        adapter_kernel,
        grid=(FSDP,),
        in_specs=[
            pl.BlockSpec((TOKENS, COLS), lambda f: (0, 0)),
            pl.BlockSpec((TOKENS, SHARD), lambda f: (0, f)),
            whole,
            whole,
        ],
        out_specs=[pl.BlockSpec((TOKENS, 2 * RANK_HALF), lambda f: (0, 0)), whole, whole],
        out_shape=[jax.ShapeDtypeStruct((TOKENS, 2 * RANK_HALF), jnp.bfloat16), packed, packed],
        scratch_shapes=[pltpu.VMEM((TOKENS, 2 * RANK_HALF), jnp.float32)],
        cost_estimate=pl.CostEstimate(
            flops=4_000_000_000, bytes_accessed=14_000_000, transcendentals=0
        ),
        name="adapter_terms",
    )(grad_out, acts, own, other)


def product_kernel(count, aliased, at_ref, *refs):
    weights, refs = refs[:count], refs[count:]
    grad_ref, mixed_ref, own_ref, other_ref = refs[:4]
    refs = refs[5:] if aliased else refs[4:]
    out_ref, held_ref, arrived = refs
    k = pl.program_id(0)

    @pl.when(k == 0)
    def _():
        for i, weight in enumerate(weights):
            pltpu.make_async_copy(weight, held_ref.at[i], arrived.at[i]).start()

    for i, weight in enumerate(weights):

        @pl.when(k == i)
        def _(i=i, weight=weight):
            pltpu.make_async_copy(weight, held_ref.at[i], arrived.at[i]).wait()

    down = jnp.concatenate([own_ref[0], other_ref[0]], axis=0)
    side = jnp.dot(mixed_ref[...], down, preferred_element_type=jnp.float32)
    base = lax.dot_general(grad_ref[...], held_ref[k], NT, preferred_element_type=jnp.float32)
    out_ref[...] = (base + adapter_scale * side).astype(jnp.bfloat16)


def product(at, weights, grad_out, mixed, own, other, target):
    count, aliased = len(weights), target is not None
    down_spec = pl.BlockSpec((1, RANK_HALF, HALF), lambda k, at: (at[k] // 2, 0, at[k] % 2))
    return pl.pallas_call(
        functools.partial(product_kernel, count, aliased),
        grid_spec=pltpu.PrefetchScalarGridSpec(
            num_scalar_prefetch=1,
            grid=(count,),
            in_specs=[pl.BlockSpec(memory_space=pl.ANY)] * count
            + [
                pl.BlockSpec((TOKENS, COLS), lambda k, at: (0, 0)),
                pl.BlockSpec((TOKENS, 2 * RANK_HALF), lambda k, at: (0, 0)),
                down_spec,
                down_spec,
            ]
            + [pl.BlockSpec(memory_space=pl.ANY)] * aliased,
            out_specs=pl.BlockSpec((TOKENS, HALF), lambda k, at: (0, at[k])),
            scratch_shapes=[
                pltpu.VMEM((count, HALF, COLS), jnp.bfloat16),
                pltpu.SemaphoreType.DMA((count,)),
            ],
        ),
        out_shape=jax.ShapeDtypeStruct((TOKENS, WIDTH), jnp.bfloat16),
        input_output_aliases={1 + count + 4: 0} if aliased else {},
        cost_estimate=pl.CostEstimate(
            flops=2 * count * TOKENS * HALF * 1100,
            bytes_accessed=count * 1_600_000 + 1_000_000,
            transcendentals=0,
        ),
        name=f"product_{count}",
    )(jnp.stack(at), *weights, grad_out, mixed, own, other, *([target] if aliased else []))


def local(acts, grad_out, codes, scale_codes, col_scale, down_adapter, up_adapter):
    y, core = lax.axis_index("y"), lax.axis_index("core")
    z, xl = lax.axis_index("z"), lax.axis_index("xl")
    step = 1 - 2 * ((core + y) % 2)

    packed = jnp.concatenate(
        [
            lax.dynamic_slice_in_dim(down_adapter, core * RANK_HALF, RANK_HALF, 0),
            lax.dynamic_slice_in_dim(up_adapter, core * RANK_HALF, RANK_HALF, 0),
        ],
        axis=1,
    )
    own = lax.all_to_all(
        jnp.broadcast_to(packed[None], (FSDP, RANK_HALF, PACKED)), ("z", "xl"), 0, 0, tiled=True
    )
    other = moved(own, core_swap)

    w = dequantized_half(jnp.reshape(core, (1,)).astype(jnp.int32), codes, scale_codes, col_scale)
    w_z1, w_x0 = moved(w, z_hop), moved(w, x_hop)
    w_z2, w_x1, w_y1 = moved(w_z1, z_hop), moved(w_z1, x_hop), moved(w_z1, y_swap)
    w_x2, w_xy = moved(w_z2, x_hop), moved(w_x1, y_swap)

    mixed, sums, sums_other = adapter_terms(grad_out, acts, own, other)

    def column(dz, cross, half):
        shard = ((z + dz + 4) % 4) * 2 + (1 - xl if cross else xl)
        return shard * 2 + half

    def at_own(dz, cross):
        return column(dz, cross, core)

    def at_other(dz, cross):
        return column(dz, cross, 1 - core)

    stages = (
        ((w, 0, 0, False),),
        ((w_z1, -step, step, False), (w_x0, 0, 0, True)),
        ((w_z2, 2, 2, False), (w_x1, -step, step, True), (w_y1, step, -step, False)),
        ((w_x2, 2, 2, True), (w_xy, step, -step, True)),
    )
    out = None
    for pieces in stages:
        at = [at_own(dz, cross) for _, dz, _, cross in pieces]
        at += [at_other(dz, cross) for _, _, dz, cross in pieces]
        weights = [piece[0] for piece in pieces]
        weights += [moved(piece, core_swap) for piece in weights]
        out = product(at, weights, grad_out, mixed, own, other, out)

    def added(parts):
        return parts.astype(jnp.float32).sum(axis=0)

    sums = (sums.astype(jnp.float32) + moved(sums_other, core_swap).astype(jnp.float32)).astype(
        jnp.bfloat16
    )
    sums = added(lax.all_to_all(sums, ("z", "xl"), 0, 0, tiled=True)).astype(jnp.bfloat16)
    sums = added(
        lax.all_to_all(
            jnp.broadcast_to(sums[None], (8, RANK_HALF, PACKED)), ("y", "xh"), 0, 0, tiled=True
        )
    )
    scale_factor = adapter_scale * float(TOKENS * DEVICES) ** (-0.5)
    mine = scale_factor * sums
    theirs = moved(mine, core_swap)
    grads = jnp.where(
        core == 0, jnp.concatenate([mine, theirs], 0), jnp.concatenate([theirs, mine], 0)
    )
    return out, grads[:, :SHARD], grads[:, SHARD:]


def solution(mesh):
    fine = Mesh(mesh.devices.reshape(SIZES), AXES)
    fsdp = ("z", "xl")
    placed = (
        P(AXES, None),
        P(AXES, None),
        P(fsdp, None, None),
        P(fsdp, None),
        P(),
        P(None, fsdp),
        P(None, fsdp),
    )
    return jax.shard_map(
        local,
        mesh=fine,
        in_specs=placed,
        out_specs=(P(AXES, None), P(None, fsdp), P(None, fsdp)),
        check_vma=False,
    )
```

```python
import functools

import jax
import jax.numpy as jnp
from jax import lax
from jax.experimental import pallas as pl
from jax.experimental.pallas import tpu as pltpu
from jax.sharding import Mesh
from jax.sharding import PartitionSpec as P


adapter_scale = 0.5
nf4_table = [
    -1.0,
    -0.6961928009986877,
    -0.5250730514526367,
    -0.39491748809814453,
    -0.28444138169288635,
    -0.18477343022823334,
    -0.09105003625154495,
    0.0,
    0.07958029955625534,
    0.16093020141124725,
    0.24611230194568634,
    0.33791524171829224,
    0.44070982933044434,
    0.5626170039176941,
    0.7229568362236023,
    1.0,
]

AXES = ("y", "xh", "core", "z", "xl")
SIZES = (4, 2, 2, 4, 2)
DEVICES = 128
HALF = 512
SHARD = 1024
WIDTH = 8192
COLS = 1024
TOKENS = 512
RANK_HALF = 32
UP = 128
PACKED = 1152


def place(device):
    rest, xl = divmod(device, 2)
    rest, z = divmod(rest, 4)
    rest, core = divmod(rest, 2)
    y, xh = divmod(rest, 2)
    return xh * 2 + xl, y, z, core


def device_at(x, y, z, core):
    return (((y * 2 + x // 2) * 2 + core) * 4 + z) * 2 + x % 2


def z_hop(x, y, z, core):
    step = 1 if (core + y) % 2 == 0 else -1
    return x, y, (z + step) % 4, core


def x_hop(x, y, z, core):
    step = 1 if core == 0 else -1
    return (x + step) % 4, y, z, core


def y_swap(x, y, z, core):
    step = 1 if (core + y) % 2 == 0 else -1
    return x, (y + step) % 4, z, core


def core_swap(x, y, z, core):
    return x, y, z, 1 - core


def moved(value, hop):
    pairs = [(d, device_at(*hop(*place(d)))) for d in range(DEVICES)]
    return lax.ppermute(value, AXES, pairs)


NT = (((1,), (1,)), ((), ()))
TN = (((0,), (0,)), ((), ()))
VMEM = pl.BlockSpec(memory_space=pltpu.VMEM)
ANY = pl.BlockSpec(memory_space=pl.ANY)
HBM = pl.BlockSpec(memory_space=pltpu.HBM)


def position():
    y, core, z, xl = (lax.axis_index(name) for name in ("y", "core", "z", "xl"))
    return y, core, z, xl


def piece_place(slot):
    y, core, _, _ = position()
    half = core if slot < 8 else 1 - core
    step = 1 - 2 * lax.rem(half + y, 2)
    ups = (0, -step, 0, 2, -step, step, 2, step)
    crosses = (0, 0, 1, 0, 1, 0, 1, 1)
    return lax.rem(ups[slot % 8] + 4, 4), crosses[slot % 8], half


def shard_at(up, cross):
    _, _, z, xl = position()
    return lax.rem(z + up, 4) * 2 + lax.rem(xl + cross, 2)


def pack_kernel(down_ref, up_ref, packed_ref):
    _, core, _, _ = position()
    ranks = pl.ds(pl.multiple_of(core * RANK_HALF, RANK_HALF), RANK_HALF)
    packed_ref[:, :SHARD] = down_ref[ranks, :]
    packed_ref[:, SHARD:] = up_ref[ranks, :]


def packed_half(down_adapter, up_adapter):
    return pl.pallas_call(
        pack_kernel,
        in_specs=[VMEM, VMEM],
        out_specs=VMEM,
        out_shape=pltpu.VMEM((RANK_HALF, PACKED), jnp.bfloat16),
        compiler_params=LIMIT,
        name="pack",
    )(down_adapter, up_adapter)


def join_kernel(mine_ref, crossed_ref, pair_ref):
    pair_ref[0] = mine_ref[...]
    pair_ref[1] = crossed_ref[...]


def joined(mine, crossed):
    return pl.pallas_call(
        join_kernel,
        in_specs=[VMEM, VMEM],
        out_specs=VMEM,
        out_shape=pltpu.VMEM((2, RANK_HALF, PACKED), jnp.bfloat16),
        compiler_params=LIMIT,
        name="join",
    )(in_vmem(mine), in_vmem(crossed))


def prepare_kernel(
    codes_ref, scale_ref, col_ref, acts_ref,
    weight_ref, held_ref, words_ref, scales_ref, rows_ref, arrived
):
    _, core, _, _ = position()
    first = pl.multiple_of(core * 8, 8)
    scales = pltpu.make_async_copy(scale_ref.at[pl.ds(first, 8)], scales_ref, arrived.at[0])
    words = [
        pltpu.make_async_copy(
            codes_ref.at[pl.ds(first + 2 * i, 2)], words_ref.at[pl.ds(2 * i, 2)], arrived.at[1 + i]
        )
        for i in range(4)
    ]
    scales.start()
    for copy in words:
        copy.start()
    acts = [
        pltpu.make_async_copy(
            acts_ref.at[i * 64 : (i + 1) * 64], held_ref.at[i * 64 : (i + 1) * 64], arrived.at[5 + i]
        )
        for i in range(8)
    ]
    scales.wait()
    for copy in acts:
        copy.start()

    def block(b):
        absmax = scales_ref[pl.ds(b, 1), :].astype(jnp.float32)
        absmax = (absmax + 1.0) / 256.0 * col_ref[...]
        for lane in range(COLS // 128):
            code = words_ref[b, :, lane * 128 : (lane + 1) * 128]
            scale = absmax[:, lane * 128 : (lane + 1) * 128]
            for j in range(4):
                bits = [(code & (1 << (4 * j + k))) != 0 for k in range(4)]
                levels = [jnp.full(code.shape, q, jnp.float32) for q in nf4_table]
                for k in range(4):
                    levels = [
                        jnp.where(bits[k], levels[i + 1], levels[i])
                        for i in range(0, len(levels), 2)
                    ]
                rows_ref[lane, pl.ds(j, 16, stride=4), :] = levels[0] * scale
        for lane in range(COLS // 128):
            weight_ref[pl.ds(pl.multiple_of(b * 64, 64), 64), lane * 128 : (lane + 1) * 128] = (
                rows_ref[lane].astype(jnp.bfloat16)
            )

    for copy in words:
        copy.wait()
    pl.loop(0, 8)(block)
    for copy in acts:
        copy.wait()


def prepared(codes, scale_codes, col_scale, acts):
    return pl.pallas_call(
        prepare_kernel,
        in_specs=[HBM, HBM, VMEM, HBM],
        out_specs=[VMEM, VMEM],
        out_shape=[
            pltpu.VMEM((HALF, COLS), jnp.bfloat16),
            pltpu.VMEM((TOKENS, WIDTH), jnp.bfloat16),
        ],
        scratch_shapes=[
            pltpu.VMEM((8, 16, COLS), jnp.int32),
            pltpu.VMEM((8, COLS), jnp.int32),
            pltpu.VMEM((COLS // 128, 64, 128), jnp.float32),
            pltpu.SemaphoreType.DMA((13,)),
        ],
        compiler_params=LIMIT,
        cost_estimate=pl.CostEstimate(
            flops=2_000_000_000, bytes_accessed=9_600_000, transcendentals=0
        ),
        name="prepare",
    )(in_hbm(codes), in_hbm(scale_codes), col_scale.reshape(1, COLS), in_hbm(acts))


def in_hbm(value):
    return pltpu.with_memory_space_constraint(value, pltpu.HBM)


def in_vmem(value):
    return pltpu.with_memory_space_constraint(value, pltpu.VMEM)


LIMIT = pltpu.CompilerParams(vmem_limit_bytes=12 * 2**20)


def adapter_kernel(grad_ref, *refs):
    own_refs, other_refs = refs[:4], refs[4:8]
    acts_ref, mixed_ref, down_ref, sums_ref, rest_ref = refs[8:]
    order = [(up, cross) for up in range(4) for cross in range(2)]

    def columns(up, cross, width):
        return pl.ds(pl.multiple_of(shard_at(up, cross) * width, width), width)

    mixed = jnp.zeros((TOKENS, 2 * RANK_HALF), jnp.float32)
    for up, cross in order:
        down_ref[up, cross, :RANK_HALF] = own_refs[up][cross, :, :SHARD]
        down_ref[up, cross, RANK_HALF:] = other_refs[up][cross, :, :SHARD]
        up_rows = jnp.concatenate(
            [own_refs[up][cross, :, SHARD:], other_refs[up][cross, :, SHARD:]], axis=0
        )
        mixed += lax.dot_general(
            grad_ref[:, columns(up, cross, UP)], up_rows, NT, preferred_element_type=jnp.float32
        )
    mixed = mixed.astype(jnp.bfloat16)
    mixed_ref[...] = mixed

    lowered = jnp.zeros((TOKENS, 2 * RANK_HALF), jnp.float32)
    for up, cross in order:
        acts = acts_ref[:, columns(up, cross, SHARD)]
        term = lax.dot_general(mixed, acts, TN, preferred_element_type=jnp.float32)
        lowered += lax.dot_general(
            acts, down_ref[up, cross], NT, preferred_element_type=jnp.float32
        )
        sums_ref[up, cross, :, :SHARD] = term[:RANK_HALF].astype(jnp.bfloat16)
        rest_ref[up, cross, :, :SHARD] = term[RANK_HALF:].astype(jnp.bfloat16)
    lowered = lowered.astype(jnp.bfloat16)
    for up, cross in order:
        term = lax.dot_general(
            lowered, grad_ref[:, columns(up, cross, UP)], TN, preferred_element_type=jnp.float32
        ).astype(jnp.bfloat16)
        sums_ref[up, cross, :, SHARD:] = term[:RANK_HALF]
        rest_ref[up, cross, :, SHARD:] = term[RANK_HALF:]


def adapter_terms(grad_out, own, other, acts):
    packed = pltpu.VMEM((4, 2, RANK_HALF, PACKED), jnp.bfloat16)
    return pl.pallas_call(
        adapter_kernel,
        in_specs=[VMEM] * 10,
        out_specs=[VMEM] * 4,
        out_shape=[
            pltpu.VMEM((TOKENS, 2 * RANK_HALF), jnp.bfloat16),
            pltpu.VMEM((4, 2, 2 * RANK_HALF, SHARD), jnp.bfloat16),
            packed,
            packed,
        ],
        compiler_params=LIMIT,
        cost_estimate=pl.CostEstimate(
            flops=5_000_000_000, bytes_accessed=12_000_000, transcendentals=0
        ),
        name="adapter",
    )(*map(in_vmem, (grad_out, *own, *other, acts)))


def two_sums_kernel(mine_ref, arrived_ref, *out_refs):
    for i, ref in enumerate(out_refs):
        ref[...] = (
            mine_ref[i].astype(jnp.float32) + arrived_ref[i].astype(jnp.float32)
        ).astype(jnp.bfloat16)


def core_sums(mine, arrived):
    shape = pltpu.VMEM((2, RANK_HALF, PACKED), jnp.bfloat16)
    return pl.pallas_call(
        two_sums_kernel,
        in_specs=[VMEM, VMEM],
        out_specs=[VMEM] * 4,
        out_shape=[shape] * 4,
        compiler_params=LIMIT,
        name="core_sums",
    )(in_vmem(mine), in_vmem(arrived))


def four_sums_kernel(split, scale, *refs):
    ins, outs = refs[:4], refs[4:]
    total = ins[0][...].astype(jnp.float32)
    for ref in ins[1:]:
        total += ref[...].astype(jnp.float32)
    if scale is not None:
        total = total * scale
    for i, ref in enumerate(outs):
        ref[...] = (total[i] if split else total).astype(ref.dtype)


def four_sums(parts, split, dtype, scale=None):
    shape = pltpu.VMEM((RANK_HALF, PACKED), dtype)
    return pl.pallas_call(
        functools.partial(four_sums_kernel, split, scale),
        in_specs=[VMEM] * 4,
        out_specs=[VMEM] * 2 if split else VMEM,
        out_shape=[shape] * 2 if split else shape,
        compiler_params=LIMIT,
    )(*map(in_vmem, parts))


def product_kernel(slots, aliased, *refs):
    count = len(slots)
    weights, refs = refs[:count], refs[count:]
    grad_ref, mixed_ref, down_ref = refs[:3]
    refs = refs[4:] if aliased else refs[3:]
    out_ref, made_ref, sent = refs

    def copy(k):
        up, cross, half = piece_place(slots[k])
        column = pl.multiple_of((shard_at(up, cross) * 2 + half) * HALF, HALF)
        return pltpu.make_async_copy(
            made_ref.at[k % 2], out_ref.at[:, pl.ds(column, HALF)], sent.at[k % 2]
        )

    for k in range(count):
        up, cross, half = piece_place(slots[k])
        down = down_ref[up, cross, :, pl.ds(pl.multiple_of(half * HALF, HALF), HALF)]
        side = jnp.dot(mixed_ref[...], down, preferred_element_type=jnp.float32)
        base = lax.dot_general(
            grad_ref[...], weights[k][...], NT, preferred_element_type=jnp.float32
        )
        if k >= 2:
            copy(k - 2).wait()
        made_ref[k % 2] = (base + adapter_scale * side).astype(jnp.bfloat16)
        copy(k).start()
    for k in range(max(0, count - 2), count):
        copy(k).wait()


def product(slots, weights, grad_out, mixed, down, target):
    count, aliased = len(weights), target is not None
    return pl.pallas_call(
        functools.partial(product_kernel, slots, aliased),
        in_specs=[VMEM] * (count + 3) + [ANY] * aliased,
        out_specs=ANY,
        out_shape=jax.ShapeDtypeStruct((TOKENS, WIDTH), jnp.bfloat16),
        scratch_shapes=[
            pltpu.VMEM((2, TOKENS, HALF), jnp.bfloat16),
            pltpu.SemaphoreType.DMA((2,)),
        ],
        input_output_aliases={count + 3: 0} if aliased else {},
        cost_estimate=pl.CostEstimate(
            flops=2 * count * TOKENS * HALF * 1100,
            bytes_accessed=count * 1_600_000 + 1_000_000,
            transcendentals=0,
        ),
        compiler_params=LIMIT,
    )(*map(in_vmem, (*weights, grad_out, mixed, down)), *([target] if aliased else []))


def final_kernel(mine_ref, theirs_ref, down_ref, up_ref):
    _, core, _, _ = position()
    for ref, half in ((mine_ref, core), (theirs_ref, 1 - core)):
        rows = pl.ds(pl.multiple_of(half * RANK_HALF, RANK_HALF), RANK_HALF)
        down_ref[rows, :] = ref[:, :SHARD]
        up_ref[rows, :] = ref[:, SHARD:]


def in_order(mine, theirs):
    return pl.pallas_call(
        final_kernel,
        in_specs=[VMEM, VMEM],
        out_specs=[VMEM, VMEM],
        out_shape=[
            jax.ShapeDtypeStruct((2 * RANK_HALF, SHARD), jnp.float32),
            jax.ShapeDtypeStruct((2 * RANK_HALF, UP), jnp.float32),
        ],
        compiler_params=LIMIT,
        name="in_order",
    )(in_vmem(mine), in_vmem(theirs))


def shifted(axis, by):
    def hop(*at):
        at = list(at)
        at["xyz".index(axis)] = (at["xyz".index(axis)] + by) % 4
        return tuple(at)

    return hop


def step(acts, grad_out, codes, scale_codes, col_scale, down_adapter, up_adapter):
    packed = packed_half(down_adapter, up_adapter)
    crossed = moved(packed, x_hop)
    w, acts = prepared(codes, scale_codes, col_scale, acts)
    pair = joined(packed, crossed)
    own, other = [pair] + [None] * 3, [None] * 4
    for dz in (1, 3, 2):
        own[4 - dz] = moved(pair, shifted("z", dz))
    for up in (0, 3, 1, 2):
        other[up] = moved(own[up], core_swap)
    w_z1 = moved(w, z_hop)
    w_x0 = moved(w, x_hop)
    w_z2 = moved(w_z1, z_hop)
    w_x1 = moved(w_z1, x_hop)
    w_y1 = moved(w_z1, y_swap)
    w_x2 = moved(w_z2, x_hop)
    w_xy = moved(w_x1, y_swap)

    mixed, down, sums, rest = adapter_terms(grad_out, own, other, acts)
    arrived = moved(rest, core_swap)
    sums = core_sums(sums, arrived)
    parts = [sums[0]]
    for dz in (1, 3, 2):
        parts.append(moved(sums[dz], shifted("z", dz)))
    mine, cross = four_sums(parts, True, jnp.bfloat16)
    parts = [mine]
    for dx, part in ((1, cross), (3, cross), (2, mine)):
        parts.append(moved(part, shifted("x", dx)))
    mine = four_sums(parts, False, jnp.bfloat16)
    parts = [mine]
    for dy in (1, 3, 2):
        parts.append(moved(mine, shifted("y", dy)))
    scale = adapter_scale * float(TOKENS * DEVICES) ** (-0.5)
    mine = four_sums(parts, False, jnp.float32, scale)

    pieces = (w, w_z1, w_x0, w_z2, w_x1, w_y1, w_x2, w_xy)
    mirrored = []
    for piece in pieces:
        mirrored.append(moved(piece, core_swap))
    out = None
    for stage in ((0,), (1, 2), (3, 4, 5), (6, 7)):
        slots = stage + tuple(8 + k for k in stage)
        weights = [pieces[k] for k in stage] + [mirrored[k] for k in stage]
        out = product(slots, weights, grad_out, mixed, down, out)

    theirs = moved(mine, core_swap)
    grad_down, grad_up = in_order(mine, theirs)
    return out, grad_down, grad_up


def solution(mesh):
    fine = Mesh(mesh.devices.reshape(SIZES), AXES)
    fsdp = ("z", "xl")
    placed = (
        P(AXES, None),
        P(AXES, None),
        P(fsdp, None, None),
        P(fsdp, None),
        P(),
        P(None, fsdp),
        P(None, fsdp),
    )
    return jax.shard_map(
        step,
        mesh=fine,
        in_specs=placed,
        out_specs=(P(AXES, None), P(None, fsdp), P(None, fsdp)),
        check_vma=False,
    )
```

```python
import functools

import jax
import jax.numpy as jnp
from jax import lax
from jax.experimental import pallas as pl
from jax.experimental.pallas import tpu as pltpu
from jax.sharding import Mesh
from jax.sharding import PartitionSpec as P


adapter_scale = 0.5
nf4_table = [
    -1.0,
    -0.6961928009986877,
    -0.5250730514526367,
    -0.39491748809814453,
    -0.28444138169288635,
    -0.18477343022823334,
    -0.09105003625154495,
    0.0,
    0.07958029955625534,
    0.16093020141124725,
    0.24611230194568634,
    0.33791524171829224,
    0.44070982933044434,
    0.5626170039176941,
    0.7229568362236023,
    1.0,
]

AXES = ("y", "xh", "core", "z", "xl")
SIZES = (4, 2, 2, 4, 2)
DEVICES = 128
HALF = 512
SHARD = 1024
WIDTH = 8192
COLS = 1024
TOKENS = 512
RANK_HALF = 32
UP = 128
PACKED = 1152


def place(device):
    rest, xl = divmod(device, 2)
    rest, z = divmod(rest, 4)
    rest, core = divmod(rest, 2)
    y, xh = divmod(rest, 2)
    return xh * 2 + xl, y, z, core


def device_at(x, y, z, core):
    return (((y * 2 + x // 2) * 2 + core) * 4 + z) * 2 + x % 2


def z_hop(x, y, z, core):
    step = 1 if (core + y) % 2 == 0 else -1
    return x, y, (z + step) % 4, core


def z_back(x, y, z, core):
    step = 1 if (core + y) % 2 == 0 else -1
    return x, y, (z - step) % 4, core


def x_hop(x, y, z, core):
    step = 1 if core == 0 else -1
    return (x + step) % 4, y, z, core


def y_swap(x, y, z, core):
    step = 1 if (core + y) % 2 == 0 else -1
    return x, (y + step) % 4, z, core


def core_swap(x, y, z, core):
    return x, y, z, 1 - core


def moved(value, hop):
    pairs = [(d, device_at(*hop(*place(d)))) for d in range(DEVICES)]
    return lax.ppermute(value, AXES, pairs)


NT = (((1,), (1,)), ((), ()))
TN = (((0,), (0,)), ((), ()))
VMEM = pl.BlockSpec(memory_space=pltpu.VMEM)
ANY = pl.BlockSpec(memory_space=pl.ANY)
HBM = pl.BlockSpec(memory_space=pltpu.HBM)


def position():
    y, core, z, xl = (lax.axis_index(name) for name in ("y", "core", "z", "xl"))
    return y, core, z, xl


def z_offsets():
    y, core, _, _ = position()
    odd = lax.rem(core + y, 2)
    return 0, 3 - 2 * odd, 1 + 2 * odd, 2


PLACES = ((0, 0), (1, 0), (0, 1), (3, 0), (1, 1), (2, 0), (3, 1), (2, 1))
MIRROR = (0, 2, 1, 3)


def piece_place(slot):
    _, core, _, _ = position()
    place, cross = PLACES[slot % 8]
    return (place, cross, core) if slot < 8 else (MIRROR[place], cross, 1 - core)


def shard_at(place, cross):
    _, _, z, xl = position()
    return lax.rem(z + z_offsets()[place], 4) * 2 + lax.rem(xl + cross, 2)


def pack_kernel(down_ref, up_ref, packed_ref, arrived):
    _, core, _, _ = position()
    ranks = pl.ds(pl.multiple_of(core * RANK_HALF, RANK_HALF), RANK_HALF)
    copies = [
        pltpu.make_async_copy(down_ref.at[ranks], packed_ref.at[:, :SHARD], arrived.at[0]),
        pltpu.make_async_copy(up_ref.at[ranks], packed_ref.at[:, SHARD:], arrived.at[1]),
    ]
    for copy in copies:
        copy.start()
    for copy in copies:
        copy.wait()


def packed_half(down_adapter, up_adapter):
    return pl.pallas_call(
        pack_kernel,
        in_specs=[HBM, HBM],
        out_specs=VMEM,
        out_shape=pltpu.VMEM((RANK_HALF, PACKED), jnp.bfloat16),
        scratch_shapes=[pltpu.SemaphoreType.DMA((2,))],
        compiler_params=LIMIT,
        name="pack",
    )(in_hbm(down_adapter), in_hbm(up_adapter))


def join_kernel(mine_ref, crossed_ref, pair_ref):
    pair_ref[0] = mine_ref[...]
    pair_ref[1] = crossed_ref[...]


def joined(mine, crossed):
    return pl.pallas_call(
        join_kernel,
        in_specs=[VMEM, VMEM],
        out_specs=VMEM,
        out_shape=pltpu.VMEM((2, RANK_HALF, PACKED), jnp.bfloat16),
        compiler_params=LIMIT,
        name="join",
    )(in_vmem(mine), in_vmem(crossed))


def prepare_kernel(
    codes_ref, scale_ref, col_ref, acts_ref,
    weight_ref, held_ref, words_ref, scales_ref, columns_ref, rows_ref, arrived
):
    _, core, _, _ = position()
    first = pl.multiple_of(core * 8, 8)
    scales = pltpu.make_async_copy(scale_ref.at[pl.ds(first, 8)], scales_ref, arrived.at[0])
    words = [
        pltpu.make_async_copy(
            codes_ref.at[pl.ds(first + 2 * i, 2)], words_ref.at[pl.ds(2 * i, 2)], arrived.at[1 + i]
        )
        for i in range(4)
    ]
    columns = pltpu.make_async_copy(col_ref, columns_ref, arrived.at[13])
    scales.start()
    columns.start()
    for copy in words:
        copy.start()
    acts = [
        pltpu.make_async_copy(
            acts_ref.at[i * 64 : (i + 1) * 64], held_ref.at[i * 64 : (i + 1) * 64], arrived.at[5 + i]
        )
        for i in range(8)
    ]
    scales.wait()
    columns.wait()
    for copy in acts:
        copy.start()

    def block(b):
        absmax = scales_ref[pl.ds(b, 1), :].astype(jnp.float32)
        absmax = (absmax + 1.0) / 256.0 * columns_ref[...]
        for lane in range(COLS // 128):
            code = words_ref[b, :, lane * 128 : (lane + 1) * 128]
            scale = absmax[:, lane * 128 : (lane + 1) * 128]
            for j in range(4):
                bits = [(code & (1 << (4 * j + k))) != 0 for k in range(4)]
                levels = [jnp.full(code.shape, q, jnp.float32) for q in nf4_table]
                for k in range(4):
                    levels = [
                        jnp.where(bits[k], levels[i + 1], levels[i])
                        for i in range(0, len(levels), 2)
                    ]
                rows_ref[lane, pl.ds(j, 16, stride=4), :] = levels[0] * scale
        for lane in range(COLS // 128):
            weight_ref[pl.ds(pl.multiple_of(b * 64, 64), 64), lane * 128 : (lane + 1) * 128] = (
                rows_ref[lane].astype(jnp.bfloat16)
            )

    for copy in words:
        copy.wait()
    pl.loop(0, 8)(block)
    for copy in acts:
        copy.wait()


def prepared(codes, scale_codes, col_scale, acts):
    return pl.pallas_call(
        prepare_kernel,
        in_specs=[HBM, HBM, HBM, HBM],
        out_specs=[VMEM, VMEM],
        out_shape=[
            pltpu.VMEM((HALF, COLS), jnp.bfloat16),
            pltpu.VMEM((TOKENS, WIDTH), jnp.bfloat16),
        ],
        scratch_shapes=[
            pltpu.VMEM((8, 16, COLS), jnp.int32),
            pltpu.VMEM((8, COLS), jnp.int32),
            pltpu.VMEM((1, COLS), jnp.float32),
            pltpu.VMEM((COLS // 128, 64, 128), jnp.float32),
            pltpu.SemaphoreType.DMA((14,)),
        ],
        compiler_params=LIMIT,
        cost_estimate=pl.CostEstimate(
            flops=2_000_000_000, bytes_accessed=9_600_000, transcendentals=0
        ),
        name="prepare",
    )(in_hbm(codes), in_hbm(scale_codes), in_hbm(col_scale.reshape(1, COLS)), in_hbm(acts))


def in_hbm(value):
    return pltpu.with_memory_space_constraint(value, pltpu.HBM)


def in_vmem(value):
    return pltpu.with_memory_space_constraint(value, pltpu.VMEM)


LIMIT = pltpu.CompilerParams(vmem_limit_bytes=12 * 2**20)


def adapter_kernel(grad_ref, *refs):
    own_refs, other_refs = refs[:4], refs[4:8]
    acts_ref, mixed_ref, down_ref, sums_ref, rest_ref = refs[8:]
    order = [(up, cross) for up in range(4) for cross in range(2)]

    def columns(up, cross, width):
        return pl.ds(pl.multiple_of(shard_at(up, cross) * width, width), width)

    mixed = jnp.zeros((TOKENS, 2 * RANK_HALF), jnp.float32)
    for up, cross in order:
        down_ref[up, cross, :RANK_HALF] = own_refs[up][cross, :, :SHARD]
        down_ref[up, cross, RANK_HALF:] = other_refs[up][cross, :, :SHARD]
        up_rows = jnp.concatenate(
            [own_refs[up][cross, :, SHARD:], other_refs[up][cross, :, SHARD:]], axis=0
        )
        mixed += lax.dot_general(
            grad_ref[:, columns(up, cross, UP)], up_rows, NT, preferred_element_type=jnp.float32
        )
    mixed = mixed.astype(jnp.bfloat16)
    mixed_ref[...] = mixed

    lowered = jnp.zeros((TOKENS, 2 * RANK_HALF), jnp.float32)
    for up, cross in order:
        acts = acts_ref[:, columns(up, cross, SHARD)]
        term = lax.dot_general(mixed, acts, TN, preferred_element_type=jnp.float32)
        lowered += lax.dot_general(
            acts, down_ref[up, cross], NT, preferred_element_type=jnp.float32
        )
        sums_ref[up, cross, :, :SHARD] = term[:RANK_HALF].astype(jnp.bfloat16)
        rest_ref[MIRROR[up], cross, :, :SHARD] = term[RANK_HALF:].astype(jnp.bfloat16)
    lowered = lowered.astype(jnp.bfloat16)
    for up, cross in order:
        term = lax.dot_general(
            lowered, grad_ref[:, columns(up, cross, UP)], TN, preferred_element_type=jnp.float32
        ).astype(jnp.bfloat16)
        sums_ref[up, cross, :, SHARD:] = term[:RANK_HALF]
        rest_ref[MIRROR[up], cross, :, SHARD:] = term[RANK_HALF:]


def adapter_terms(grad_out, own, other, acts):
    packed = pltpu.VMEM((4, 2, RANK_HALF, PACKED), jnp.bfloat16)
    return pl.pallas_call(
        adapter_kernel,
        in_specs=[VMEM] * 10,
        out_specs=[VMEM] * 4,
        out_shape=[
            pltpu.VMEM((TOKENS, 2 * RANK_HALF), jnp.bfloat16),
            pltpu.VMEM((4, 2, 2 * RANK_HALF, SHARD), jnp.bfloat16),
            packed,
            packed,
        ],
        compiler_params=LIMIT,
        cost_estimate=pl.CostEstimate(
            flops=5_000_000_000, bytes_accessed=12_000_000, transcendentals=0
        ),
        name="adapter",
    )(*map(in_vmem, (grad_out, *own, *other, acts)))


def two_sums_kernel(mine_ref, arrived_ref, *out_refs):
    for i, ref in enumerate(out_refs):
        ref[...] = (
            mine_ref[i].astype(jnp.float32) + arrived_ref[i].astype(jnp.float32)
        ).astype(jnp.bfloat16)


def core_sums(mine, arrived):
    shape = pltpu.VMEM((2, RANK_HALF, PACKED), jnp.bfloat16)
    return pl.pallas_call(
        two_sums_kernel,
        in_specs=[VMEM, VMEM],
        out_specs=[VMEM] * 4,
        out_shape=[shape] * 4,
        compiler_params=LIMIT,
        name="core_sums",
    )(in_vmem(mine), in_vmem(arrived))


def sums_kernel(split, scale, count, *refs):
    ins, outs = refs[:count], refs[count:]
    total = ins[0][...].astype(jnp.float32)
    for ref in ins[1:]:
        total += ref[...].astype(jnp.float32)
    if scale is not None:
        total = total * scale
    for i, ref in enumerate(outs):
        ref[...] = (total[i] if split else total).astype(ref.dtype)


def sums_of(parts, dtype, split=False, scale=None):
    shape = pltpu.VMEM(parts[0].shape[1:] if split else parts[0].shape, dtype)
    return pl.pallas_call(
        functools.partial(sums_kernel, split, scale, len(parts)),
        in_specs=[VMEM] * len(parts),
        out_specs=[VMEM] * 2 if split else VMEM,
        out_shape=[shape] * 2 if split else shape,
        compiler_params=LIMIT,
    )(*map(in_vmem, parts))


def product_kernel(slots, aliased, *refs):
    count = len(slots)
    weights, refs = refs[:count], refs[count:]
    grad_ref, mixed_ref, down_ref = refs[:3]
    refs = refs[4:] if aliased else refs[3:]
    out_ref, made_ref, sent = refs

    def copy(k):
        up, cross, half = piece_place(slots[k])
        column = pl.multiple_of((shard_at(up, cross) * 2 + half) * HALF, HALF)
        return pltpu.make_async_copy(
            made_ref.at[k % 2], out_ref.at[:, pl.ds(column, HALF)], sent.at[k % 2]
        )

    for k in range(count):
        up, cross, half = piece_place(slots[k])
        down = down_ref[up, cross, :, pl.ds(pl.multiple_of(half * HALF, HALF), HALF)]
        side = jnp.dot(mixed_ref[...], down, preferred_element_type=jnp.float32)
        base = lax.dot_general(
            grad_ref[...], weights[k][...], NT, preferred_element_type=jnp.float32
        )
        if k >= 2:
            copy(k - 2).wait()
        made_ref[k % 2] = (base + adapter_scale * side).astype(jnp.bfloat16)
        copy(k).start()
    for k in range(max(0, count - 2), count):
        copy(k).wait()


def product(slots, weights, grad_out, mixed, down, target):
    count, aliased = len(weights), target is not None
    return pl.pallas_call(
        functools.partial(product_kernel, slots, aliased),
        in_specs=[VMEM] * (count + 3) + [ANY] * aliased,
        out_specs=ANY,
        out_shape=jax.ShapeDtypeStruct((TOKENS, WIDTH), jnp.bfloat16),
        scratch_shapes=[
            pltpu.VMEM((2, TOKENS, HALF), jnp.bfloat16),
            pltpu.SemaphoreType.DMA((2,)),
        ],
        input_output_aliases={count + 3: 0} if aliased else {},
        cost_estimate=pl.CostEstimate(
            flops=2 * count * TOKENS * HALF * 1100,
            bytes_accessed=count * 1_600_000 + 1_000_000,
            transcendentals=0,
        ),
        compiler_params=LIMIT,
    )(*map(in_vmem, (*weights, grad_out, mixed, down)), *([target] if aliased else []))


def final_kernel(mine_ref, theirs_ref, down_ref, up_ref):
    _, core, _, _ = position()
    for ref, half in ((mine_ref, core), (theirs_ref, 1 - core)):
        rows = pl.ds(pl.multiple_of(half * RANK_HALF, RANK_HALF), RANK_HALF)
        down_ref[rows, :] = ref[:, :SHARD]
        up_ref[rows, :] = ref[:, SHARD:]


def in_order(mine, theirs):
    return pl.pallas_call(
        final_kernel,
        in_specs=[VMEM, VMEM],
        out_specs=[VMEM, VMEM],
        out_shape=[
            jax.ShapeDtypeStruct((2 * RANK_HALF, SHARD), jnp.float32),
            jax.ShapeDtypeStruct((2 * RANK_HALF, UP), jnp.float32),
        ],
        compiler_params=LIMIT,
        name="in_order",
    )(in_vmem(mine), in_vmem(theirs))


def shifted(axis, by):
    def hop(*at):
        at = list(at)
        at["xyz".index(axis)] = (at["xyz".index(axis)] + by) % 4
        return tuple(at)

    return hop


def step(acts, grad_out, codes, scale_codes, col_scale, down_adapter, up_adapter):
    packed = packed_half(down_adapter, up_adapter)
    crossed = moved(packed, x_hop)
    w, acts = prepared(codes, scale_codes, col_scale, acts)
    pair = joined(packed, crossed)
    ahead = moved(pair, z_back)
    behind = moved(pair, z_hop)
    far = moved(ahead, z_back)
    own = (pair, behind, ahead, far)
    other = [None] * 4
    for place in range(4):
        other[MIRROR[place]] = moved(own[place], core_swap)
    w_z1 = moved(w, z_hop)
    w_x0 = moved(w, x_hop)
    w_z2 = moved(w_z1, z_hop)
    w_x1 = moved(w_z1, x_hop)
    w_y1 = moved(w_z1, y_swap)
    w_x2 = moved(w_z2, x_hop)
    w_xy = moved(w_x1, y_swap)

    mixed, down, sums, rest = adapter_terms(grad_out, own, other, acts)
    arrived = moved(rest, core_swap)
    sums = core_sums(sums, arrived)
    relayed = moved(sums[3], z_back)
    behind = moved(sums[2], z_hop)
    relayed = sums_of((sums[1], relayed), jnp.bfloat16)
    ahead = moved(relayed, z_back)
    mine, cross = sums_of((sums[0], behind, ahead), jnp.bfloat16, split=True)
    parts = [mine]
    for by, part in ((1, cross), (3, cross), (2, mine)):
        parts.append(moved(part, shifted("x", by)))
    mine = sums_of(parts, jnp.bfloat16)
    parts = [mine]
    for by in (1, 3, 2):
        parts.append(moved(mine, shifted("y", by)))
    scale = adapter_scale * float(TOKENS * DEVICES) ** (-0.5)
    mine = sums_of(parts, jnp.float32, scale=scale)

    pieces = (w, w_z1, w_x0, w_z2, w_x1, w_y1, w_x2, w_xy)
    mirrored = []
    for piece in pieces:
        mirrored.append(moved(piece, core_swap))
    out = None
    turns = ((0, 8), (1, 2, 9, 10), (3, 4, 5, 11, 12, 13), (6, 7), (14, 15))
    everything = (*pieces, *mirrored)
    for slots in turns:
        weights = [everything[k] for k in slots]
        out = product(slots, weights, grad_out, mixed, down, out)

    theirs = moved(mine, core_swap)
    grad_down, grad_up = in_order(mine, theirs)
    return out, grad_down, grad_up


def solution(mesh):
    fine = Mesh(mesh.devices.reshape(SIZES), AXES)
    fsdp = ("z", "xl")
    placed = (
        P(AXES, None),
        P(AXES, None),
        P(fsdp, None, None),
        P(fsdp, None),
        P(),
        P(None, fsdp),
        P(None, fsdp),
    )
    return jax.shard_map(
        step,
        mesh=fine,
        in_specs=placed,
        out_specs=(P(AXES, None), P(None, fsdp), P(None, fsdp)),
        check_vma=False,
    )
```

```python
import functools

import jax
import jax.numpy as jnp
from jax import lax
from jax.experimental import pallas as pl
from jax.experimental.pallas import tpu as pltpu
from jax.sharding import Mesh
from jax.sharding import PartitionSpec as P


adapter_scale = 0.5
nf4_table = [
    -1.0,
    -0.6961928009986877,
    -0.5250730514526367,
    -0.39491748809814453,
    -0.28444138169288635,
    -0.18477343022823334,
    -0.09105003625154495,
    0.0,
    0.07958029955625534,
    0.16093020141124725,
    0.24611230194568634,
    0.33791524171829224,
    0.44070982933044434,
    0.5626170039176941,
    0.7229568362236023,
    1.0,
]

AXES = ("y", "xh", "core", "z", "xl")
SIZES = (4, 2, 2, 4, 2)
DEVICES = 128
HALF = 512
SHARD = 1024
WIDTH = 8192
COLS = 1024
TOKENS = 512
RANK_HALF = 32
UP = 128
PACKED = 1152


def place(device):
    rest, xl = divmod(device, 2)
    rest, z = divmod(rest, 4)
    rest, core = divmod(rest, 2)
    y, xh = divmod(rest, 2)
    return xh * 2 + xl, y, z, core


def device_at(x, y, z, core):
    return (((y * 2 + x // 2) * 2 + core) * 4 + z) * 2 + x % 2


def z_hop(x, y, z, core):
    step = 1 if (core + y) % 2 == 0 else -1
    return x, y, (z + step) % 4, core


def z_back(x, y, z, core):
    step = 1 if (core + y) % 2 == 0 else -1
    return x, y, (z - step) % 4, core


def x_hop(x, y, z, core):
    step = 1 if core == 0 else -1
    return (x + step) % 4, y, z, core


def y_swap(x, y, z, core):
    step = 1 if (core + y) % 2 == 0 else -1
    return x, (y + step) % 4, z, core


def y_other(x, y, z, core):
    step = -1 if (core + y) % 2 == 0 else 1
    return x, (y + step) % 4, z, core


def core_swap(x, y, z, core):
    return x, y, z, 1 - core


def moved(value, hop):
    pairs = [(d, device_at(*hop(*place(d)))) for d in range(DEVICES)]
    return lax.ppermute(value, AXES, pairs)


NT = (((1,), (1,)), ((), ()))
TN = (((0,), (0,)), ((), ()))
VMEM = pl.BlockSpec(memory_space=pltpu.VMEM)
ANY = pl.BlockSpec(memory_space=pl.ANY)
HBM = pl.BlockSpec(memory_space=pltpu.HBM)


def position():
    y, core, z, xl = (lax.axis_index(name) for name in ("y", "core", "z", "xl"))
    return y, core, z, xl


def z_offsets():
    y, core, _, _ = position()
    odd = lax.rem(core + y, 2)
    return 0, 3 - 2 * odd, 1 + 2 * odd, 2


PLACES = ((0, 0), (1, 0), (0, 1), (3, 0), (1, 1), (2, 0), (3, 1), (2, 1))
MIRROR = (0, 2, 1, 3)


def piece_place(slot):
    _, core, _, _ = position()
    place, cross = PLACES[slot % 8]
    return (place, cross, core) if slot < 8 else (MIRROR[place], cross, 1 - core)


def shard_at(place, cross):
    _, _, z, xl = position()
    return lax.rem(z + z_offsets()[place], 4) * 2 + lax.rem(xl + cross, 2)


def pack_kernel(down_ref, up_ref, packed_ref, arrived):
    _, core, _, _ = position()
    ranks = pl.ds(pl.multiple_of(core * RANK_HALF, RANK_HALF), RANK_HALF)
    copies = [
        pltpu.make_async_copy(down_ref.at[ranks], packed_ref.at[:, :SHARD], arrived.at[0]),
        pltpu.make_async_copy(up_ref.at[ranks], packed_ref.at[:, SHARD:], arrived.at[1]),
    ]
    for copy in copies:
        copy.start()
    for copy in copies:
        copy.wait()


def packed_half(down_adapter, up_adapter):
    return pl.pallas_call(
        pack_kernel,
        in_specs=[HBM, HBM],
        out_specs=VMEM,
        out_shape=pltpu.VMEM((RANK_HALF, PACKED), jnp.bfloat16),
        scratch_shapes=[pltpu.SemaphoreType.DMA((2,))],
        compiler_params=LIMIT,
        name="pack",
    )(in_hbm(down_adapter), in_hbm(up_adapter))


def join_kernel(mine_ref, crossed_ref, pair_ref):
    pair_ref[0] = mine_ref[...]
    pair_ref[1] = crossed_ref[...]


def joined(mine, crossed):
    return pl.pallas_call(
        join_kernel,
        in_specs=[VMEM, VMEM],
        out_specs=VMEM,
        out_shape=pltpu.VMEM((2, RANK_HALF, PACKED), jnp.bfloat16),
        compiler_params=LIMIT,
        name="join",
    )(in_vmem(mine), in_vmem(crossed))


def prepare_kernel(
    codes_ref, scale_ref, col_ref, acts_ref,
    weight_ref, held_ref, words_ref, scales_ref, columns_ref, rows_ref, arrived
):
    _, core, _, _ = position()
    first = pl.multiple_of(core * 8, 8)
    scales = pltpu.make_async_copy(scale_ref.at[pl.ds(first, 8)], scales_ref, arrived.at[0])
    words = [
        pltpu.make_async_copy(
            codes_ref.at[pl.ds(first + 2 * i, 2)], words_ref.at[pl.ds(2 * i, 2)], arrived.at[1 + i]
        )
        for i in range(4)
    ]
    columns = pltpu.make_async_copy(col_ref, columns_ref, arrived.at[13])
    scales.start()
    columns.start()
    for copy in words:
        copy.start()
    acts = [
        pltpu.make_async_copy(
            acts_ref.at[i * 64 : (i + 1) * 64], held_ref.at[i * 64 : (i + 1) * 64], arrived.at[5 + i]
        )
        for i in range(8)
    ]
    scales.wait()
    columns.wait()
    for copy in acts:
        copy.start()

    def block(b):
        absmax = scales_ref[pl.ds(b, 1), :].astype(jnp.float32)
        absmax = (absmax + 1.0) / 256.0 * columns_ref[...]
        for lane in range(COLS // 128):
            code = words_ref[b, :, lane * 128 : (lane + 1) * 128]
            scale = absmax[:, lane * 128 : (lane + 1) * 128]
            for j in range(4):
                bits = [(code & (1 << (4 * j + k))) != 0 for k in range(4)]
                levels = [jnp.full(code.shape, q, jnp.float32) for q in nf4_table]
                for k in range(4):
                    levels = [
                        jnp.where(bits[k], levels[i + 1], levels[i])
                        for i in range(0, len(levels), 2)
                    ]
                rows_ref[lane, pl.ds(j, 16, stride=4), :] = levels[0] * scale
        for lane in range(COLS // 128):
            weight_ref[pl.ds(pl.multiple_of(b * 64, 64), 64), lane * 128 : (lane + 1) * 128] = (
                rows_ref[lane].astype(jnp.bfloat16)
            )

    for copy in words:
        copy.wait()
    pl.loop(0, 8)(block)
    for copy in acts:
        copy.wait()


def prepared(codes, scale_codes, col_scale, acts):
    return pl.pallas_call(
        prepare_kernel,
        in_specs=[HBM, HBM, HBM, HBM],
        out_specs=[VMEM, VMEM],
        out_shape=[
            pltpu.VMEM((HALF, COLS), jnp.bfloat16),
            pltpu.VMEM((TOKENS, WIDTH), jnp.bfloat16),
        ],
        scratch_shapes=[
            pltpu.VMEM((8, 16, COLS), jnp.int32),
            pltpu.VMEM((8, COLS), jnp.int32),
            pltpu.VMEM((1, COLS), jnp.float32),
            pltpu.VMEM((COLS // 128, 64, 128), jnp.float32),
            pltpu.SemaphoreType.DMA((14,)),
        ],
        compiler_params=LIMIT,
        cost_estimate=pl.CostEstimate(
            flops=2_000_000_000, bytes_accessed=9_600_000, transcendentals=0
        ),
        name="prepare",
    )(in_hbm(codes), in_hbm(scale_codes), in_hbm(col_scale.reshape(1, COLS)), in_hbm(acts))


def in_hbm(value):
    return pltpu.with_memory_space_constraint(value, pltpu.HBM)


def in_vmem(value):
    return pltpu.with_memory_space_constraint(value, pltpu.VMEM)


LIMIT = pltpu.CompilerParams(vmem_limit_bytes=12 * 2**20)


def adapter_kernel(grad_ref, *refs):
    own_refs, other_refs = refs[:4], refs[4:8]
    acts_ref, mixed_ref, down_ref, sums_ref, rest_ref = refs[8:]
    order = [(up, cross) for up in range(4) for cross in range(2)]

    def columns(up, cross, width):
        return pl.ds(pl.multiple_of(shard_at(up, cross) * width, width), width)

    mixed = jnp.zeros((TOKENS, 2 * RANK_HALF), jnp.float32)
    for up, cross in order:
        down_ref[up, cross, :RANK_HALF] = own_refs[up][cross, :, :SHARD]
        down_ref[up, cross, RANK_HALF:] = other_refs[up][cross, :, :SHARD]
        up_rows = jnp.concatenate(
            [own_refs[up][cross, :, SHARD:], other_refs[up][cross, :, SHARD:]], axis=0
        )
        mixed += lax.dot_general(
            grad_ref[:, columns(up, cross, UP)], up_rows, NT, preferred_element_type=jnp.float32
        )
    mixed = mixed.astype(jnp.bfloat16)
    mixed_ref[...] = mixed

    lowered = jnp.zeros((TOKENS, 2 * RANK_HALF), jnp.float32)
    for up, cross in order:
        acts = acts_ref[:, columns(up, cross, SHARD)]
        term = lax.dot_general(mixed, acts, TN, preferred_element_type=jnp.float32)
        lowered += lax.dot_general(
            acts, down_ref[up, cross], NT, preferred_element_type=jnp.float32
        )
        sums_ref[up, cross, :, :SHARD] = term[:RANK_HALF].astype(jnp.bfloat16)
        rest_ref[MIRROR[up], cross, :, :SHARD] = term[RANK_HALF:].astype(jnp.bfloat16)
    lowered = lowered.astype(jnp.bfloat16)
    for up, cross in order:
        term = lax.dot_general(
            lowered, grad_ref[:, columns(up, cross, UP)], TN, preferred_element_type=jnp.float32
        ).astype(jnp.bfloat16)
        sums_ref[up, cross, :, SHARD:] = term[:RANK_HALF]
        rest_ref[MIRROR[up], cross, :, SHARD:] = term[RANK_HALF:]


def adapter_terms(grad_out, own, other, acts):
    packed = pltpu.VMEM((4, 2, RANK_HALF, PACKED), jnp.bfloat16)
    return pl.pallas_call(
        adapter_kernel,
        in_specs=[VMEM] * 10,
        out_specs=[VMEM] * 4,
        out_shape=[
            pltpu.VMEM((TOKENS, 2 * RANK_HALF), jnp.bfloat16),
            pltpu.VMEM((4, 2, 2 * RANK_HALF, SHARD), jnp.bfloat16),
            packed,
            packed,
        ],
        compiler_params=LIMIT,
        cost_estimate=pl.CostEstimate(
            flops=5_000_000_000, bytes_accessed=12_000_000, transcendentals=0
        ),
        name="adapter",
    )(*map(in_vmem, (grad_out, *own, *other, acts)))


def two_sums_kernel(mine_ref, arrived_ref, *out_refs):
    for i, ref in enumerate(out_refs):
        ref[...] = (
            mine_ref[i].astype(jnp.float32) + arrived_ref[i].astype(jnp.float32)
        ).astype(jnp.bfloat16)


def core_sums(mine, arrived):
    shape = pltpu.VMEM((2, RANK_HALF, PACKED), jnp.bfloat16)
    return pl.pallas_call(
        two_sums_kernel,
        in_specs=[VMEM, VMEM],
        out_specs=[VMEM] * 4,
        out_shape=[shape] * 4,
        compiler_params=LIMIT,
        name="core_sums",
    )(in_vmem(mine), in_vmem(arrived))


def sums_kernel(split, scale, count, *refs):
    ins, outs = refs[:count], refs[count:]
    total = ins[0][...].astype(jnp.float32)
    for ref in ins[1:]:
        total += ref[...].astype(jnp.float32)
    if scale is not None:
        total = total * scale
    for i, ref in enumerate(outs):
        ref[...] = (total[i] if split else total).astype(ref.dtype)


def sums_of(parts, dtype, split=False, scale=None):
    shape = pltpu.VMEM(parts[0].shape[1:] if split else parts[0].shape, dtype)
    return pl.pallas_call(
        functools.partial(sums_kernel, split, scale, len(parts)),
        in_specs=[VMEM] * len(parts),
        out_specs=[VMEM] * 2 if split else VMEM,
        out_shape=[shape] * 2 if split else shape,
        compiler_params=LIMIT,
    )(*map(in_vmem, parts))


def product_kernel(slots, aliased, *refs):
    count = len(slots)
    weights, refs = refs[:count], refs[count:]
    grad_ref, mixed_ref, down_ref = refs[:3]
    refs = refs[4:] if aliased else refs[3:]
    out_ref, made_ref, sent = refs

    def copy(k):
        up, cross, half = piece_place(slots[k])
        column = pl.multiple_of((shard_at(up, cross) * 2 + half) * HALF, HALF)
        return pltpu.make_async_copy(
            made_ref.at[k % 2], out_ref.at[:, pl.ds(column, HALF)], sent.at[k % 2]
        )

    for k in range(count):
        up, cross, half = piece_place(slots[k])
        down = down_ref[up, cross, :, pl.ds(pl.multiple_of(half * HALF, HALF), HALF)]
        side = jnp.dot(mixed_ref[...], down, preferred_element_type=jnp.float32)
        base = lax.dot_general(
            grad_ref[...], weights[k][...], NT, preferred_element_type=jnp.float32
        )
        if k >= 2:
            copy(k - 2).wait()
        made_ref[k % 2] = (base + adapter_scale * side).astype(jnp.bfloat16)
        copy(k).start()
    for k in range(max(0, count - 2), count):
        copy(k).wait()


def product(slots, weights, grad_out, mixed, down, target):
    count, aliased = len(weights), target is not None
    return pl.pallas_call(
        functools.partial(product_kernel, slots, aliased),
        in_specs=[VMEM] * (count + 3) + [ANY] * aliased,
        out_specs=ANY,
        out_shape=jax.ShapeDtypeStruct((TOKENS, WIDTH), jnp.bfloat16),
        scratch_shapes=[
            pltpu.VMEM((2, TOKENS, HALF), jnp.bfloat16),
            pltpu.SemaphoreType.DMA((2,)),
        ],
        input_output_aliases={count + 3: 0} if aliased else {},
        cost_estimate=pl.CostEstimate(
            flops=2 * count * TOKENS * HALF * 1100,
            bytes_accessed=count * 1_600_000 + 1_000_000,
            transcendentals=0,
        ),
        compiler_params=LIMIT,
    )(*map(in_vmem, (*weights, grad_out, mixed, down)), *([target] if aliased else []))


def final_kernel(mine_ref, theirs_ref, down_ref, up_ref):
    _, core, _, _ = position()
    for ref, half in ((mine_ref, core), (theirs_ref, 1 - core)):
        rows = pl.ds(pl.multiple_of(half * RANK_HALF, RANK_HALF), RANK_HALF)
        down_ref[rows, :] = ref[:, :SHARD]
        up_ref[rows, :] = ref[:, SHARD:]


def in_order(mine, theirs):
    return pl.pallas_call(
        final_kernel,
        in_specs=[VMEM, VMEM],
        out_specs=[VMEM, VMEM],
        out_shape=[
            jax.ShapeDtypeStruct((2 * RANK_HALF, SHARD), jnp.float32),
            jax.ShapeDtypeStruct((2 * RANK_HALF, UP), jnp.float32),
        ],
        compiler_params=LIMIT,
        name="in_order",
    )(in_vmem(mine), in_vmem(theirs))


def shifted(axis, by):
    def hop(*at):
        at = list(at)
        at["xyz".index(axis)] = (at["xyz".index(axis)] + by) % 4
        return tuple(at)

    return hop


def step(acts, grad_out, codes, scale_codes, col_scale, down_adapter, up_adapter):
    packed = packed_half(down_adapter, up_adapter)
    crossed = moved(packed, x_hop)
    w, acts = prepared(codes, scale_codes, col_scale, acts)
    pair = joined(packed, crossed)
    ahead = moved(pair, z_back)
    behind = moved(pair, z_hop)
    far = moved(ahead, z_back)
    own = (pair, behind, ahead, far)
    other = [None] * 4
    for place in range(4):
        other[MIRROR[place]] = moved(own[place], core_swap)
    w_z1 = moved(w, z_hop)
    w_x0 = moved(w, x_hop)
    w_z2 = moved(w_z1, z_hop)
    w_x1 = moved(w_z1, x_hop)
    w_y1 = moved(w_z1, y_swap)
    w_x2 = moved(w_z2, x_hop)
    w_xy = moved(w_x1, y_swap)

    mixed, down, sums, rest = adapter_terms(grad_out, own, other, acts)
    arrived = moved(rest, core_swap)
    sums = core_sums(sums, arrived)
    relayed = moved(sums[3], z_back)
    behind = moved(sums[2], z_hop)
    relayed = sums_of((sums[1], relayed), jnp.bfloat16)
    ahead = moved(relayed, z_back)
    mine, cross = sums_of((sums[0], behind, ahead), jnp.bfloat16, split=True)
    parts = [mine]
    for by, part in ((1, cross), (3, cross), (2, mine)):
        parts.append(moved(part, shifted("x", by)))
    mine = sums_of(parts, jnp.bfloat16)
    arrived = moved(mine, y_other)
    mine = sums_of((mine, arrived), jnp.bfloat16)
    arrived = moved(mine, y_swap)
    scale = adapter_scale * float(TOKENS * DEVICES) ** (-0.5)
    mine = sums_of((mine, arrived), jnp.float32, scale=scale)

    pieces = (w, w_z1, w_x0, w_z2, w_x1, w_y1, w_x2, w_xy)
    mirrored = []
    for piece in pieces:
        mirrored.append(moved(piece, core_swap))
    out = None
    turns = ((0, 8), (1, 2, 9, 10), (3, 4, 5, 11, 12, 13), (6, 7), (14, 15))
    everything = (*pieces, *mirrored)
    for slots in turns:
        weights = [everything[k] for k in slots]
        out = product(slots, weights, grad_out, mixed, down, out)

    theirs = moved(mine, core_swap)
    grad_down, grad_up = in_order(mine, theirs)
    return out, grad_down, grad_up


def solution(mesh):
    fine = Mesh(mesh.devices.reshape(SIZES), AXES)
    fsdp = ("z", "xl")
    placed = (
        P(AXES, None),
        P(AXES, None),
        P(fsdp, None, None),
        P(fsdp, None),
        P(),
        P(None, fsdp),
        P(None, fsdp),
    )
    return jax.shard_map(
        step,
        mesh=fine,
        in_specs=placed,
        out_specs=(P(AXES, None), P(None, fsdp), P(None, fsdp)),
        check_vma=False,
    )
```
